32 devices in a mesh: grp: 2 (over core), dev: 16 (over z, y, x).
Axes of the slice: x: 2, y: 2, z: 4, core: 2. Of those that a mesh axis runs over, the one named last changes fastest.
Arguments:
- tokens: bfloat16 [2048, 2048], P('dev', 'grp'), may hold values from -6 to 6
- gate_up: bfloat16 [2048, 2, 16, 7168], P('dev', None, None, 'grp'), may hold values from -0.125 to 0.125
- down: bfloat16 [16, 7168, 2048], P('dev', 'grp'), may hold values from -0.046875 to 0.046875
- expert_ids: int32 [2048, 2], P('dev'), may hold values from 0 to 7, all different within a row; in each aligned block of 128 rows (0 to 127, 128 to 255, ...) at most 40 rows name the same one
- gate_num: int32 [2048, 2], P('dev'), may hold values from 1 to 15
Outputs:
- moe_out: bfloat16 [2048, 2048], P('dev', 'grp')
The draws below stay inside these ranges and needn't reach their ends.
Inputs may be any that keep to these rules, and one draw needn't show every extreme that they name: `expert_ids`: each row names 2 different experts. In each aligned block of 128 rows no expert is named by more than 40 rows, a bound that some block reaches.
All inputs are finite; a program needn't handle non-finite values.
Results may differ from the reference program's by a relative error of at most 0.0083.
Values may be sent and summed in bfloat16 or wider, within the bound.
A program may use at most 192 MiB of HBM per device.

```python
import math
import jax
import jax.numpy as jnp
import numpy as np

D = 2048
FF = 14336
EXPERTS = 8
TOP = 2
TOK_DEV = 128
CAP = 40
COLS = 2
TOKENS = 2048
N_DEV = 16


def with_ends(array, key, smallest, top_value):
    place = [jax.random.randint(jax.random.fold_in(key, axis), (), 0, length) for axis, length in enumerate(array.shape)]
    widest = array.shape.index(max(array.shape))
    next_to = place[:widest] + [(place[widest] + 1) % array.shape[widest]] + place[widest + 1:]
    return array.at[tuple(place)].set(smallest).at[tuple(next_to)].set(top_value)


def block_levels(rng, extent, pieces, smallest, high):
    def one(position, blocks):
        heights = jax.random.uniform(jax.random.fold_in(jax.random.fold_in(rng, 6), position), (blocks,), jnp.float32, smallest / len(pieces), high / len(pieces))
        return jnp.repeat(jnp.exp(heights), extent[position] // blocks).reshape((-1,) + (1,) * (len(extent) - position - 1))

    loudness = one(*pieces[0])
    for cut in pieces[1:]:
        loudness = loudness * one(*cut)
    return loudness


def deal_out(stream_key, own, number, rows, count, top, bound, slope):
    sequence = jax.random.permutation(stream_key, count)
    crowded, usual = load_shares(count, rows * top, bound, slope, True), load_shares(count, rows * top, bound, slope, False)
    places = jnp.arange(count)

    def named(tallies, offset_by):
        used = int((tallies > 0).sum())
        fixed = max(1, used // 4)
        passed = fixed + (places - fixed + offset_by * (used - fixed)) % max(1, count - fixed)
        return jnp.zeros((count,), jnp.int32).at[sequence[jnp.where(places < fixed, places, passed)]].set(jnp.asarray(tallies, jnp.int32))

    tallies = jnp.where(number % 4 == 0, named(crowded, number // 4), named(usual, number - number // 4 - 1))
    mixed = jax.random.permutation(jax.random.fold_in(own, 3), count)
    donor, sink = mixed[0:count // 2 * 2:2], mixed[1:count // 2 * 2:2]
    slack = jnp.minimum(tallies[donor] - 1, bound - tallies[sink]) // 2
    slack = jnp.where((donor == sequence[0]) | (sink == sequence[0]) | (tallies[sink] == 0), 0, jnp.maximum(slack, 0))
    passed = jax.random.randint(jax.random.fold_in(own, 4), (count // 2,), 0, 1 << 20) % (slack + 1)
    tallies = tallies.at[donor].add(-passed).at[sink].add(passed)
    items = jnp.searchsorted(jnp.cumsum(tallies), jnp.arange(rows * top), side="right").astype(jnp.int32)
    grid = items.reshape(top, rows).T
    grid = grid[jax.random.permutation(jax.random.fold_in(own, 1), rows)]
    offset_by = jax.random.randint(jax.random.fold_in(own, 2), (rows, 1), 0, top)
    return jnp.take_along_axis(grid, (jnp.arange(top)[None, :] + offset_by) % top, axis=1)


def load_shares(count, total, most, slope, full):
    portions = [(1 << 20) // math.isqrt(standing ** slope) + 1 for standing in range(1, count + 1)]
    largest = most if full else min(most, max(-(-total // count), total * portions[0] // sum(portions)))
    least = 1 if total - largest >= count - 1 else 0
    holding, rest = [largest] + [least] * (count - 1), total - largest - least * (count - 1)
    while rest > 0:
        movable = [i for i in range(1, count) if holding[i] < largest] or [i for i in range(1, count) if holding[i] < most]
        whole, left = sum([portions[i] for i in movable]), rest
        for i in movable:
            addition = min(most - holding[i], max(1, left * portions[i] // whole), rest)
            holding[i] = holding[i] + addition
            rest = rest - addition
    return np.array(holding)


def scatter_about(key, shape, spread, reach, cuts=(), kind=jnp.bfloat16):
    gain = block_levels(key, shape, cuts, -0.22, 0.18) if cuts else 1.0
    values = jax.random.normal(key, shape, jnp.float32) * spread * gain
    return jnp.minimum(jnp.maximum(values, -reach), reach).astype(kind)


def setup_inputs(seed: int = 0) -> dict:
    keys = jax.random.split(jax.random.key(seed), 6)
    tokens = scatter_about(keys[0], (TOKENS, D), 1.0, 6.0, ((0, 16), (1, 2)))
    gate_up = scatter_about(keys[1], (D, 2, EXPERTS * COLS, FF // COLS), D ** -0.5, 0.125, ((0, 16), (3, 2)))
    down = scatter_about(keys[2], (EXPERTS * COLS, FF // COLS, D), FF ** -0.5, 0.046875, ((0, 16), (1, 2)))
    expert_ids_keys = jax.random.split(jax.random.fold_in(keys[3], 1), TOKENS // TOK_DEV)
    expert_ids_turns = jax.random.permutation(jax.random.fold_in(keys[3], 3), TOKENS // TOK_DEV)
    expert_ids = jax.vmap(lambda own, number: deal_out(jax.random.fold_in(keys[3], 2), own, number, TOK_DEV, EXPERTS, TOP, CAP, 1))(expert_ids_keys, expert_ids_turns).reshape((TOKENS, TOP))
    gate_num = with_ends(jax.random.randint(keys[4], (TOKENS, TOP), 1, 16), jax.random.fold_in(keys[4], 1), 1, 15).astype(jnp.int32)
    return {"tokens": tokens, "gate_up": gate_up, "down": down, "expert_ids": expert_ids, "gate_num": gate_num}


def reference(tokens, gate_up, down, expert_ids, gate_num):
    gate_cols = gate_up[:, 0].reshape(D, EXPERTS, FF)
    up_cols = gate_up[:, 1].reshape(D, EXPERTS, FF)
    down_rows = down.reshape(EXPERTS, FF, D)
    numerators = gate_num.astype(jnp.float32)
    shares = numerators / jnp.sum(numerators, axis=1, keepdims=True)
    total = jnp.zeros((TOKENS, D), jnp.float32)
    limit = N_DEV * CAP
    for expert in range(EXPERTS):
        matched = expert_ids == expert
        weights = jnp.sum(jnp.where(matched, shares, jnp.zeros_like(shares)), axis=1)
        routed = jnp.any(matched, axis=1).astype(jnp.int32)
        order = jnp.argsort(1 - routed, stable=True)[:limit].astype(jnp.int32)
        chosen = tokens[order]
        gate_act = jnp.dot(chosen, gate_cols[:, expert], preferred_element_type=jnp.float32)
        up_act = jnp.dot(chosen, up_cols[:, expert], preferred_element_type=jnp.float32)
        hidden = (jax.nn.silu(gate_act) * up_act).astype(jnp.bfloat16)
        result = jnp.dot(hidden, down_rows[expert], preferred_element_type=jnp.float32)
        total = total.at[order].add(weights[order][:, None] * result)
    return total.astype(jnp.bfloat16)
```

```python
import functools

import jax
import jax.numpy as jnp
from jax import lax
from jax.experimental import pallas as pl
from jax.experimental.pallas import tpu as pltpu
from jax.sharding import PartitionSpec as P

EXPERTS = 8
TOP = 2
CAP = 40
MESH = pl.DeviceIdType.MESH


def expert_kernel(
    n,
    chunks,
    tile,
    routed_ref,
    weights_ref,
    down_ref,
    keep_ref,
    give_ref,
    rows,
    landed,
    down_rows,
    send_sem,
    recv_sem,
    own_sem,
    row_sem,
    row_send_sem,
    row_recv_sem,
    down_sem,
):
    core = lax.axis_index("grp")
    me = lax.axis_index("dev")
    depth = weights_ref.shape[2]
    width = weights_ref.shape[3] // chunks
    half = rows.shape[2]
    total = rows.shape[1]

    barrier = pltpu.get_barrier_semaphore()

    def greet(step, carry):
        pl.semaphore_signal(
            barrier, inc=1, device_id=(core, lax.rem(me + step, n)), device_id_type=MESH
        )
        return carry

    lax.fori_loop(1, n, greet, 0)
    pl.semaphore_signal(barrier, inc=1, device_id=(1 - core, me), device_id_type=MESH)
    pl.semaphore_wait(barrier, n)

    across = pltpu.make_async_remote_copy(
        src_ref=routed_ref,
        dst_ref=rows.at[core],
        send_sem=row_send_sem,
        recv_sem=row_recv_sem,
        device_id=(1 - core, me),
        device_id_type=MESH,
    )
    across.start()
    here = pltpu.make_async_copy(routed_ref, rows.at[core], row_sem)
    here.start()

    def columns(chunk):
        return pl.ds(pl.multiple_of(chunk * width, width), width)

    def place(owner):
        return pl.ds(pl.multiple_of(owner * depth, depth), depth)

    def send_chunk(chunk, carry):
        def send(step, inner):
            target = lax.rem(me + step, n)
            pltpu.make_async_remote_copy(
                src_ref=weights_ref.at[target, :, :, columns(chunk)],
                dst_ref=landed.at[chunk, :, place(me), :],
                send_sem=send_sem.at[chunk],
                recv_sem=recv_sem.at[chunk],
                device_id=(core, target),
                device_id_type=MESH,
            ).start()
            return inner

        lax.fori_loop(1, n, send, 0)
        pltpu.make_async_copy(
            weights_ref.at[me, :, :, columns(chunk)],
            landed.at[chunk, :, place(me), :],
            own_sem.at[chunk],
        ).start()
        return carry

    lax.fori_loop(0, chunks, send_chunk, 0)

    down_copies = []
    for part in range(2):
        side = core if part == 0 else 1 - core
        copy = pltpu.make_async_copy(
            down_ref.at[0, :, pl.ds(pl.multiple_of(side * half, half), half)],
            down_rows.at[part],
            down_sem.at[part],
        )
        copy.start()
        down_copies.append(copy)
    keep_ref[...] = jnp.zeros_like(keep_ref)
    give_ref[...] = jnp.zeros_like(give_ref)
    here.wait()
    across.wait()
    for copy in down_copies:
        copy.wait()

    def others(chunk):
        return landed.at[chunk, :, pl.ds(0, (n - 1) * depth), :]

    def compute(chunk, carry):
        pltpu.make_async_copy(
            landed.at[chunk, :, place(me), :], landed.at[chunk, :, place(me), :], own_sem.at[chunk]
        ).wait()
        pltpu.make_async_copy(others(chunk), others(chunk), recv_sem.at[chunk]).wait()

        def block(index, inner):
            at = pl.ds(pl.multiple_of(index * tile, tile), tile)

            def project(which):
                low = jnp.dot(
                    rows[0, at, :], landed[chunk, which, :half, :], preferred_element_type=jnp.float32
                )
                return low + jnp.dot(
                    rows[1, at, :], landed[chunk, which, half:, :], preferred_element_type=jnp.float32
                )

            gate = project(0)
            up = project(1)
            hidden = (gate / (1.0 + jnp.exp(-gate)) * up).astype(jnp.bfloat16)
            below = pl.ds(pl.multiple_of(chunk * width, width), width)
            keep_ref[at, :] += jnp.dot(
                hidden, down_rows[0, below, :], preferred_element_type=jnp.float32
            )
            give_ref[at, :] += jnp.dot(
                hidden, down_rows[1, below, :], preferred_element_type=jnp.float32
            )
            return inner

        return lax.fori_loop(0, total // tile, block, carry)

    lax.fori_loop(0, chunks, compute, 0)

    def finish(chunk, carry):
        pltpu.make_async_copy(others(chunk), others(chunk), send_sem.at[chunk]).wait()
        return carry

    lax.fori_loop(0, chunks, finish, 0)


def chunk_count(width):
    for count in (7, 4, 2):
        if width % (count * 128) == 0:
            return count
    return 1


def local(tokens, gate_up, down, expert_ids, gate_num):
    shards = lax.axis_size("dev")
    column_count = shards // EXPERTS
    tok_rows = tokens.shape[0]
    half_width = tokens.shape[1]
    depth, _, _, width = gate_up.shape
    flat_ids = expert_ids.reshape(-1)
    onehot = (flat_ids[:, None] == jnp.arange(EXPERTS, dtype=jnp.int32)[None, :]).astype(jnp.int32)
    earlier = jnp.cumsum(onehot, axis=0) - onehot
    slot_index = jnp.sum(earlier * onehot, axis=1)
    positions = (flat_ids * CAP + slot_index).reshape(tok_rows, TOP)
    numerators = gate_num.astype(jnp.float32)
    shares = numerators / jnp.sum(numerators, axis=1, keepdims=True)
    places = jnp.arange(EXPERTS * CAP, dtype=jnp.int32)
    matches = places[:, None, None] == positions[None, :, :]
    select = jnp.any(matches, axis=2).astype(jnp.bfloat16)
    combine = jnp.sum(jnp.where(matches, shares[None, :, :], 0.0), axis=2)

    outgoing = jnp.dot(select, tokens, preferred_element_type=jnp.float32).astype(jnp.bfloat16)
    copies = jnp.broadcast_to(
        outgoing.reshape(EXPERTS, 1, CAP, half_width), (EXPERTS, column_count, CAP, half_width)
    )
    received = lax.all_to_all(
        copies.reshape(shards, CAP, half_width), "dev", split_axis=0, concat_axis=0, tiled=True
    )
    total = shards * CAP
    chunks = chunk_count(width)
    by_target = jnp.transpose(gate_up, (2, 1, 0, 3))
    any_space = pl.BlockSpec(memory_space=pl.ANY)
    vmem_space = pl.BlockSpec(memory_space=pltpu.VMEM)
    flops = 2 * total * 3 * width * 2 * half_width
    keep, give = pl.pallas_call(
        functools.partial(expert_kernel, shards, chunks, EXPERTS * CAP),
        out_shape=[jax.ShapeDtypeStruct((total, half_width), jnp.float32)] * 2,
        in_specs=[any_space] * 3,
        out_specs=[vmem_space] * 2,
        scratch_shapes=[
            pltpu.VMEM((2, total, half_width), jnp.bfloat16),
            pltpu.VMEM((chunks, 2, shards * depth, width // chunks), jnp.bfloat16),
            pltpu.VMEM((2, width, half_width), jnp.bfloat16),
            pltpu.SemaphoreType.DMA((chunks,)),
            pltpu.SemaphoreType.DMA((chunks,)),
            pltpu.SemaphoreType.DMA((chunks,)),
            pltpu.SemaphoreType.DMA,
            pltpu.SemaphoreType.DMA,
            pltpu.SemaphoreType.DMA,
            pltpu.SemaphoreType.DMA((2,)),
        ],
        compiler_params=pltpu.CompilerParams(
            collective_id=0, has_side_effects=True, vmem_limit_bytes=67043328
        ),
        cost_estimate=pl.CostEstimate(
            flops=flops, bytes_accessed=2 * by_target.size * 2, transcendentals=total * width
        ),
    )(received.reshape(total, half_width), by_target, down)
    summed = keep + lax.ppermute(give, "grp", [(0, 1), (1, 0)])
    returned = lax.all_to_all(
        summed.astype(jnp.bfloat16).reshape(shards, CAP, half_width),
        "dev",
        split_axis=0,
        concat_axis=0,
        tiled=True,
    )
    expert_out = jnp.sum(
        returned.reshape(EXPERTS, column_count, CAP, half_width).astype(jnp.float32), axis=1
    ).reshape(EXPERTS * CAP, half_width)
    combined = jnp.dot(
        combine.T, expert_out, preferred_element_type=jnp.float32, precision=lax.Precision.HIGHEST
    )
    return combined.astype(jnp.bfloat16)


def solution(mesh):
    in_specs = (
        P("dev", "grp"),
        P("dev", None, None, "grp"),
        P("dev", "grp", None),
        P("dev", None),
        P("dev", None),
    )
    out_specs = P("dev", "grp")
    return jax.shard_map(local, mesh=mesh, in_specs=in_specs, out_specs=out_specs, check_vma=False)
```

```python
import functools

import jax
import jax.numpy as jnp
from jax import lax
from jax.experimental import pallas as pl
from jax.experimental.pallas import tpu as pltpu
from jax.sharding import PartitionSpec as P

EXPERTS = 8
TOP = 2
CAP = 40
MESH = pl.DeviceIdType.MESH


def expert_kernel(
    n,
    chunks,
    tile,
    routed_ref,
    weights_ref,
    down_ref,
    keep_ref,
    give_ref,
    rows,
    landed,
    down_rows,
    send_sem,
    recv_sem,
    own_sem,
    row_sem,
    row_send_sem,
    row_recv_sem,
    down_sem,
):
    core = lax.axis_index("grp")
    me = lax.axis_index("dev")
    depth = weights_ref.shape[2]
    width = weights_ref.shape[3] // chunks
    half = rows.shape[2]
    total = rows.shape[1]

    barrier = pltpu.get_barrier_semaphore()

    def greet(step, carry):
        pl.semaphore_signal(
            barrier, inc=1, device_id=(core, lax.rem(me + step, n)), device_id_type=MESH
        )
        return carry

    lax.fori_loop(1, n, greet, 0)
    pl.semaphore_signal(barrier, inc=1, device_id=(1 - core, me), device_id_type=MESH)
    pl.semaphore_wait(barrier, n)

    across = pltpu.make_async_remote_copy(
        src_ref=routed_ref,
        dst_ref=rows.at[core],
        send_sem=row_send_sem,
        recv_sem=row_recv_sem,
        device_id=(1 - core, me),
        device_id_type=MESH,
    )
    across.start()
    here = pltpu.make_async_copy(routed_ref, rows.at[core], row_sem)
    here.start()

    def columns(chunk):
        return pl.ds(pl.multiple_of(chunk * width, width), width)

    def place(owner):
        return pl.ds(pl.multiple_of(owner * depth, depth), depth)

    def partner(step):
        plane = lax.rem(me // 4 + step // 4, n // 4)
        return plane * 4 + lax.rem(me // 2 + step // 2, 2) * 2 + lax.rem(me + step, 2)

    def send_chunk(chunk, carry):
        def send(step, inner):
            target = partner(step)
            pltpu.make_async_remote_copy(
                src_ref=weights_ref.at[target, :, :, columns(chunk)],
                dst_ref=landed.at[chunk, :, place(me), :],
                send_sem=send_sem.at[chunk],
                recv_sem=recv_sem.at[chunk],
                device_id=(core, target),
                device_id_type=MESH,
            ).start()
            return inner

        lax.fori_loop(1, n, send, 0)
        pltpu.make_async_copy(
            weights_ref.at[me, :, :, columns(chunk)],
            landed.at[chunk, :, place(me), :],
            own_sem.at[chunk],
        ).start()
        return carry

    lax.fori_loop(0, chunks, send_chunk, 0)

    down_copies = []
    for part in range(2):
        side = core if part == 0 else 1 - core
        copy = pltpu.make_async_copy(
            down_ref.at[0, :, pl.ds(pl.multiple_of(side * half, half), half)],
            down_rows.at[part],
            down_sem.at[part],
        )
        copy.start()
        down_copies.append(copy)
    keep_ref[...] = jnp.zeros_like(keep_ref)
    give_ref[...] = jnp.zeros_like(give_ref)
    here.wait()
    across.wait()
    for copy in down_copies:
        copy.wait()

    def others(chunk):
        return landed.at[chunk, :, pl.ds(0, (n - 1) * depth), :]

    def compute(chunk, carry):
        pltpu.make_async_copy(
            landed.at[chunk, :, place(me), :], landed.at[chunk, :, place(me), :], own_sem.at[chunk]
        ).wait()
        pltpu.make_async_copy(others(chunk), others(chunk), recv_sem.at[chunk]).wait()

        def block(index, inner):
            at = pl.ds(pl.multiple_of(index * tile, tile), tile)

            def project(which):
                low = jnp.dot(
                    rows[0, at, :], landed[chunk, which, :half, :], preferred_element_type=jnp.float32
                )
                return low + jnp.dot(
                    rows[1, at, :], landed[chunk, which, half:, :], preferred_element_type=jnp.float32
                )

            gate = project(0)
            up = project(1)
            hidden = (gate / (1.0 + jnp.exp(-gate)) * up).astype(jnp.bfloat16)
            below = pl.ds(pl.multiple_of(chunk * width, width), width)
            keep_ref[at, :] += jnp.dot(
                hidden, down_rows[0, below, :], preferred_element_type=jnp.float32
            )
            give_ref[at, :] += jnp.dot(
                hidden, down_rows[1, below, :], preferred_element_type=jnp.float32
            )
            return inner

        return lax.fori_loop(0, total // tile, block, carry)

    lax.fori_loop(0, chunks, compute, 0)

    def finish(chunk, carry):
        pltpu.make_async_copy(others(chunk), others(chunk), send_sem.at[chunk]).wait()
        return carry

    lax.fori_loop(0, chunks, finish, 0)


def chunk_count(width):
    for count in (7, 4, 2):
        if width % (count * 128) == 0:
            return count
    return 1


def local(tokens, gate_up, down, expert_ids, gate_num):
    shards = lax.axis_size("dev")
    column_count = shards // EXPERTS
    tok_rows = tokens.shape[0]
    half_width = tokens.shape[1]
    depth, _, _, width = gate_up.shape
    flat_ids = expert_ids.reshape(-1)
    onehot = (flat_ids[:, None] == jnp.arange(EXPERTS, dtype=jnp.int32)[None, :]).astype(jnp.int32)
    earlier = jnp.cumsum(onehot, axis=0) - onehot
    slot_index = jnp.sum(earlier * onehot, axis=1)
    positions = (flat_ids * CAP + slot_index).reshape(tok_rows, TOP)
    numerators = gate_num.astype(jnp.float32)
    shares = numerators / jnp.sum(numerators, axis=1, keepdims=True)
    places = jnp.arange(EXPERTS * CAP, dtype=jnp.int32)
    matches = places[:, None, None] == positions[None, :, :]
    select = jnp.any(matches, axis=2).astype(jnp.bfloat16)
    combine = jnp.sum(jnp.where(matches, shares[None, :, :], 0.0), axis=2)

    outgoing = jnp.dot(select, tokens, preferred_element_type=jnp.float32).astype(jnp.bfloat16)
    copies = jnp.broadcast_to(
        outgoing.reshape(EXPERTS, 1, CAP, half_width), (EXPERTS, column_count, CAP, half_width)
    )
    received = lax.all_to_all(
        copies.reshape(shards, CAP, half_width), "dev", split_axis=0, concat_axis=0, tiled=True
    )
    total = shards * CAP
    chunks = chunk_count(width)
    by_target = jnp.transpose(gate_up, (2, 1, 0, 3))
    any_space = pl.BlockSpec(memory_space=pl.ANY)
    vmem_space = pl.BlockSpec(memory_space=pltpu.VMEM)
    flops = 2 * total * 3 * width * 2 * half_width
    keep, give = pl.pallas_call(
        functools.partial(expert_kernel, shards, chunks, EXPERTS * CAP),
        out_shape=[jax.ShapeDtypeStruct((total, half_width), jnp.float32)] * 2,
        in_specs=[any_space] * 3,
        out_specs=[vmem_space] * 2,
        scratch_shapes=[
            pltpu.VMEM((2, total, half_width), jnp.bfloat16),
            pltpu.VMEM((chunks, 2, shards * depth, width // chunks), jnp.bfloat16),
            pltpu.VMEM((2, width, half_width), jnp.bfloat16),
            pltpu.SemaphoreType.DMA((chunks,)),
            pltpu.SemaphoreType.DMA((chunks,)),
            pltpu.SemaphoreType.DMA((chunks,)),
            pltpu.SemaphoreType.DMA,
            pltpu.SemaphoreType.DMA,
            pltpu.SemaphoreType.DMA,
            pltpu.SemaphoreType.DMA((2,)),
        ],
        compiler_params=pltpu.CompilerParams(
            collective_id=0, has_side_effects=True, vmem_limit_bytes=67043328
        ),
        cost_estimate=pl.CostEstimate(
            flops=flops, bytes_accessed=2 * by_target.size * 2, transcendentals=total * width
        ),
    )(received.reshape(total, half_width), by_target, down)
    summed = keep + lax.ppermute(give, "grp", [(0, 1), (1, 0)])
    returned = lax.all_to_all(
        summed.astype(jnp.bfloat16).reshape(shards, CAP, half_width),
        "dev",
        split_axis=0,
        concat_axis=0,
        tiled=True,
    )
    expert_out = jnp.sum(
        returned.reshape(EXPERTS, column_count, CAP, half_width).astype(jnp.float32), axis=1
    ).reshape(EXPERTS * CAP, half_width)
    combined = jnp.dot(
        combine.T, expert_out, preferred_element_type=jnp.float32, precision=lax.Precision.HIGHEST
    )
    return combined.astype(jnp.bfloat16)


def solution(mesh):
    in_specs = (
        P("dev", "grp"),
        P("dev", None, None, "grp"),
        P("dev", "grp", None),
        P("dev", None),
        P("dev", None),
    )
    out_specs = P("dev", "grp")
    return jax.shard_map(local, mesh=mesh, in_specs=in_specs, out_specs=out_specs, check_vma=False)
```
